16 devices in a mesh: data: 4 (over z, y), seq: 4 (over x, core).
Axes of the slice: x: 2, y: 2, z: 2, core: 2. Of those that a mesh axis runs over, the one named last changes fastest.
Arguments:
- x_in: bfloat16 [16, 2048, 2048], P(None, ('data', 'seq')), parts along dimension 1
- positions: int32 [2048], P(('data', 'seq')), parts along dimension 0
- w_query: bfloat16 [3, 2048, 32, 64], replicated
- w_key: bfloat16 [3, 2048, 4, 64], replicated
- w_value: bfloat16 [3, 2048, 4, 64], replicated
- w_out: bfloat16 [3, 32, 64, 2048], replicated
- w_up: bfloat16 [3, 2048, 5632], replicated
- w_down: bfloat16 [3, 5632, 2048], replicated
- g_attn: float32 [3, 2048], replicated
- g_mlp: float32 [3, 2048], replicated
Outputs:
- output: bfloat16 [16, 2048, 2048], P(None, ('data', 'seq')), parts along dimension 1
There are 4 independent parts. The reference program is written for one: setup_inputs(seed, part) draws one part's arguments, and reference() takes and returns one part's arrays. A program takes and returns all parts, laid end to end along the dimension named above; an argument that names none is the same for every part.
All inputs are finite; a program needn't handle non-finite values.
Results may differ from the reference program's by a relative error of at most 0.0166372.
Values are sent between devices in bfloat16 or wider.
A program may use at most 1 GiB of HBM per device.

```python
import jax
import jax.numpy as jnp
from jax import lax

BATCH_SIZE = 16
SEQ_LEN = 512
D_MODEL = 2048
N_HEADS = 32
N_KV_HEADS = 4
HEAD_DIM = 64
FF_DIM = 5632
N_LAYERS = 3
REF_BLOCK = 64

ROPE_BASE = 10000.0
NORM_EPS = 1e-6


def normal_weights(rng_key, w_shape, fan_in, w_gain):
    return (jax.random.normal(rng_key, w_shape, jnp.float32) * (w_gain * fan_in ** -0.5)).astype(jnp.bfloat16)


def setup_inputs(seed: int = 0, part: int = 0) -> dict:
    base_key = jax.random.key(seed)
    part_keys = jax.random.split(jax.random.fold_in(base_key, part), 6)
    weight_keys = jax.random.split(jax.random.fold_in(base_key, 100003), 8)
    step_frac = jnp.arange(SEQ_LEN, dtype=jnp.float32) / SEQ_LEN
    wave_freq = jax.random.uniform(part_keys[0], (BATCH_SIZE, 4), jnp.float32, minval=0.5, maxval=3.0)
    wave_phase = jax.random.uniform(part_keys[1], (BATCH_SIZE, 4), jnp.float32, minval=0.0, maxval=6.283185)
    wave_vals = jnp.cos(6.283185 * wave_freq[:, :, None] * step_frac[None, None, :] + wave_phase[:, :, None])
    wave_dirs = jax.random.normal(part_keys[2], (BATCH_SIZE, 4, D_MODEL), jnp.float32)
    smooth = jnp.einsum("bjs,bjd->bsd", wave_vals, wave_dirs) * 0.5
    noise_part = jax.random.normal(part_keys[3], (BATCH_SIZE, SEQ_LEN, D_MODEL), jnp.float32) * 0.7
    offset = jax.random.randint(part_keys[4], (), 0, SEQ_LEN)
    pos_gaps = jax.random.randint(part_keys[5], (SEQ_LEN,), 1, 5)
    return {
        "x_in": (smooth + noise_part).astype(jnp.bfloat16),
        "positions": (offset + jnp.cumsum(pos_gaps)).astype(jnp.int32),
        "w_query": normal_weights(weight_keys[0], (N_LAYERS, D_MODEL, N_HEADS, HEAD_DIM), D_MODEL, 1.25),
        "w_key": normal_weights(weight_keys[1], (N_LAYERS, D_MODEL, N_KV_HEADS, HEAD_DIM), D_MODEL, 1.25),
        "w_value": normal_weights(weight_keys[2], (N_LAYERS, D_MODEL, N_KV_HEADS, HEAD_DIM), D_MODEL, 1.0),
        "w_out": normal_weights(weight_keys[3], (N_LAYERS, N_HEADS, HEAD_DIM, D_MODEL), N_HEADS * HEAD_DIM, 1.0),
        "w_up": normal_weights(weight_keys[4], (N_LAYERS, D_MODEL, FF_DIM), D_MODEL, 1.0),
        "w_down": normal_weights(weight_keys[5], (N_LAYERS, FF_DIM, D_MODEL), FF_DIM, 1.0),
        "g_attn": jax.random.uniform(weight_keys[6], (N_LAYERS, D_MODEL), jnp.float32, minval=0.5, maxval=1.5),
        "g_mlp": jax.random.uniform(weight_keys[7], (N_LAYERS, D_MODEL), jnp.float32, minval=0.5, maxval=1.5),
    }


def rms_norm(x_act, gain_vec):
    x_f32 = x_act.astype(jnp.float32)
    mean_sq = jnp.mean(x_f32 * x_f32, axis=-1, keepdims=True)
    return (x_f32 * lax.rsqrt(mean_sq + NORM_EPS) * gain_vec).astype(jnp.bfloat16)


def rope_tables(positions):
    inv_freq = ROPE_BASE ** (-jnp.arange(HEAD_DIM // 2, dtype=jnp.float32) * (2.0 / HEAD_DIM))
    angles = positions.astype(jnp.float32)[:, None] * inv_freq[None, :]
    return jnp.cos(angles), jnp.sin(angles)


def apply_rope(proj_f32, cos_t, sin_t):
    half_dim = HEAD_DIM // 2
    x_first = proj_f32[..., :half_dim]
    x_second = proj_f32[..., half_dim:]
    cos_b = cos_t[:, None, :]
    sin_b = sin_t[:, None, :]
    return jnp.concatenate([x_first * cos_b - x_second * sin_b, x_second * cos_b + x_first * sin_b], axis=-1).astype(jnp.bfloat16)


def causal_attention(q_heads, k_heads, v_heads):
    groups = N_HEADS // N_KV_HEADS
    n_blocks = SEQ_LEN // REF_BLOCK
    att_scale = HEAD_DIM ** -0.5
    q_grouped = q_heads.reshape(BATCH_SIZE, SEQ_LEN, N_KV_HEADS, groups, HEAD_DIM)
    k_f32 = k_heads.astype(jnp.float32)
    v_f32 = v_heads.astype(jnp.float32)
    key_pos = jnp.arange(SEQ_LEN)

    def one_block(blk_idx):
        blk_start = blk_idx * REF_BLOCK
        q_blk = lax.dynamic_slice_in_dim(q_grouped, blk_start, REF_BLOCK, axis=1).astype(jnp.float32)
        scores = jnp.einsum("bqkgd,bskd->bkgqs", q_blk, k_f32) * att_scale
        query_pos = blk_start + jnp.arange(REF_BLOCK)
        allowed = key_pos[None, :] <= query_pos[:, None]
        scores = jnp.where(allowed, scores, -1e30)
        row_max = jnp.max(scores, axis=-1, keepdims=True)
        exp_f32 = jnp.exp(scores - row_max)
        row_sum = jnp.sum(exp_f32, axis=-1)
        weighted = jnp.einsum("bkgqs,bskd->bqkgd", exp_f32.astype(jnp.bfloat16).astype(jnp.float32), v_f32)
        return (weighted / jnp.transpose(row_sum, (0, 3, 1, 2))[..., None]).astype(jnp.bfloat16)

    blocks = lax.map(one_block, jnp.arange(n_blocks))
    return jnp.moveaxis(blocks, 0, 1).reshape(BATCH_SIZE, SEQ_LEN, N_HEADS, HEAD_DIM)


def transformer_layer(hidden, cos_t, sin_t, layer_weights):
    w_query, w_key, w_value, w_out, w_up, w_down, gain_attn, gain_mlp = layer_weights
    n_rows = BATCH_SIZE * SEQ_LEN
    normed = rms_norm(hidden, gain_attn).reshape(n_rows, D_MODEL)
    q_proj = jnp.dot(normed, w_query.reshape(D_MODEL, N_HEADS * HEAD_DIM), preferred_element_type=jnp.float32)
    k_proj = jnp.dot(normed, w_key.reshape(D_MODEL, N_KV_HEADS * HEAD_DIM), preferred_element_type=jnp.float32)
    v_proj = jnp.dot(normed, w_value.reshape(D_MODEL, N_KV_HEADS * HEAD_DIM), preferred_element_type=jnp.float32)
    q_heads = apply_rope(q_proj.reshape(BATCH_SIZE, SEQ_LEN, N_HEADS, HEAD_DIM), cos_t, sin_t)
    k_heads = apply_rope(k_proj.reshape(BATCH_SIZE, SEQ_LEN, N_KV_HEADS, HEAD_DIM), cos_t, sin_t)
    v_heads = v_proj.astype(jnp.bfloat16).reshape(BATCH_SIZE, SEQ_LEN, N_KV_HEADS, HEAD_DIM)
    attn_out = causal_attention(q_heads, k_heads, v_heads)
    attn_proj = jnp.dot(attn_out.reshape(n_rows, N_HEADS * HEAD_DIM), w_out.reshape(N_HEADS * HEAD_DIM, D_MODEL), preferred_element_type=jnp.float32)
    resid_h = (hidden.reshape(n_rows, D_MODEL).astype(jnp.float32) + attn_proj).astype(jnp.bfloat16)
    normed_mlp = rms_norm(resid_h, gain_mlp)
    gelu_act = jax.nn.gelu(jnp.dot(normed_mlp, w_up, preferred_element_type=jnp.float32), approximate=True).astype(jnp.bfloat16)
    layer_out = resid_h.astype(jnp.float32) + jnp.dot(gelu_act, w_down, preferred_element_type=jnp.float32)
    return layer_out.astype(jnp.bfloat16).reshape(BATCH_SIZE, SEQ_LEN, D_MODEL)


def reference(x_in, positions, w_query, w_key, w_value, w_out, w_up, w_down, g_attn, g_mlp):
    cos_t, sin_t = rope_tables(positions)

    def layer_body(hidden, layer_weights):
        return transformer_layer(hidden, cos_t, sin_t, layer_weights), None

    stacked = (w_query, w_key, w_value, w_out, w_up, w_down, g_attn, g_mlp)
    return lax.scan(layer_body, x_in, stacked)[0]
```

```python
import functools

import jax
import jax.numpy as jnp
from jax import lax
from jax.experimental import pallas as pl
from jax.experimental.pallas import tpu as pltpu
from jax.sharding import PartitionSpec as P

ROPE_BASE = 10000.0
NORM_EPS = 1e-6
LOG2E = 1.4426950408889634
F32 = jnp.float32
BF16 = jnp.bfloat16
NT = (((1,), (1,)), ((), ()))
VMEM_LIMIT = 64 * 1024 * 1024 - 65536


def params(limit=VMEM_LIMIT):
    return pltpu.CompilerParams(dimension_semantics=("arbitrary",), vmem_limit_bytes=limit)


def cost(flops, nbytes):
    return pl.CostEstimate(flops=int(flops), bytes_accessed=int(nbytes), transcendentals=0)


def normed(x_bf16, gain):
    x = x_bf16.astype(F32)
    mean_sq = jnp.mean(x * x, axis=-1, keepdims=True)
    return (x * lax.rsqrt(mean_sq + NORM_EPS) * gain).astype(BF16)


def rope_t(u, cos, sin):
    half = u.shape[0] // 2
    a, b = u[:half], u[half:]
    return jnp.concatenate([a * cos - b * sin, b * cos + a * sin], axis=0).astype(BF16)


def kv_body(head_dim, batch_rows, x_ref, g_ref, wk_ref, wv_ref, cos_ref, sin_ref, n_ref, k_ref, v_ref):
    n = normed(x_ref[...], g_ref[0])
    n_ref[...] = n
    k_t = lax.dot_general(wk_ref[0], n, NT, preferred_element_type=F32)
    v_t = lax.dot_general(wv_ref[0], n, NT, preferred_element_type=F32).astype(BF16)
    for i in range(n.shape[0] // batch_rows):
        cols = slice(i * batch_rows, (i + 1) * batch_rows)
        heads = [rope_t(k_t[h:h + head_dim, cols], cos_ref[...], sin_ref[...]) for h in range(0, k_t.shape[0], head_dim)]
        k_ref[i] = jnp.concatenate(heads, axis=0).T
        v_ref[i] = v_t[:, cols]


def kv_proj(layer, x, gain, wk, wv, cos, sin, head_dim, n_batch, tile=256):
    rows, d = x.shape
    kv = wk.shape[1]
    s = rows // n_batch
    per = tile // s
    return pl.pallas_call(
        functools.partial(kv_body, head_dim, s),
        grid=(rows // tile,),
        in_specs=[
            pl.BlockSpec((tile, d), lambda i: (i, 0)),
            pl.BlockSpec((1, 1, d), lambda i: (layer, 0, 0)),
            pl.BlockSpec((1, kv, d), lambda i: (layer, 0, 0)),
            pl.BlockSpec((1, kv, d), lambda i: (layer, 0, 0)),
            pl.BlockSpec(cos.shape, lambda i: (0, 0)),
            pl.BlockSpec(cos.shape, lambda i: (0, 0)),
        ],
        out_specs=[
            pl.BlockSpec((tile, d), lambda i: (i, 0)),
            pl.BlockSpec((per, s, kv), lambda i: (i, 0, 0)),
            pl.BlockSpec((per, kv, s), lambda i: (i, 0, 0)),
        ],
        out_shape=[
            jax.ShapeDtypeStruct((rows, d), BF16),
            jax.ShapeDtypeStruct((n_batch, s, kv), BF16),
            jax.ShapeDtypeStruct((n_batch, kv, s), BF16),
        ],
        compiler_params=params(),
        cost_estimate=cost(4 * rows * d * kv, 4 * rows * d),
        name=f"kv_proj",
    )(x, gain, wk, wv, cos, sin)


def q_body(head_dim, batch_rows, fchunk, n_ref, wq_ref, cos_ref, sin_ref, q_ref):
    feats = wq_ref.shape[1]
    for f0 in range(0, feats, fchunk):
        u = lax.dot_general(wq_ref[0, f0:f0 + fchunk, :], n_ref[...], NT, preferred_element_type=F32)
        for i in range(n_ref.shape[0] // batch_rows):
            cols = slice(i * batch_rows, (i + 1) * batch_rows)
            for h in range(0, fchunk, head_dim):
                q_ref[i, f0 + h:f0 + h + head_dim, :] = rope_t(u[h:h + head_dim, cols], cos_ref[...], sin_ref[...])


def q_proj(layer, n, wq, cos, sin, head_dim, n_batch, tile=256, fchunk=512):
    rows, d = n.shape
    feats = wq.shape[1]
    s = rows // n_batch
    per = tile // s
    return pl.pallas_call(
        functools.partial(q_body, head_dim, s, fchunk),
        grid=(rows // tile,),
        in_specs=[
            pl.BlockSpec((tile, d), lambda i: (i, 0)),
            pl.BlockSpec((1, feats, d), lambda i: (layer, 0, 0), pipeline_mode=pl.Buffered(1)),
            pl.BlockSpec(cos.shape, lambda i: (0, 0)),
            pl.BlockSpec(cos.shape, lambda i: (0, 0)),
        ],
        out_specs=pl.BlockSpec((per, feats, s), lambda i: (i, 0, 0)),
        out_shape=jax.ShapeDtypeStruct((n_batch, feats, s), BF16),
        compiler_params=params(),
        cost_estimate=cost(2 * rows * d * feats, 4 * rows * d + 2 * feats * d),
        name="q_proj",
    )(n, wq, cos, sin)


def attn_one(head_dim, n_kv, chunk, q_ref, k_refs, v_refs, o_ref):
    s = q_ref.shape[2]
    groups = q_ref.shape[1] // head_dim // n_kv
    factor = LOG2E * head_dim ** -0.5
    row = lax.broadcasted_iota(jnp.int32, (s, chunk * s), 0)
    col = lax.broadcasted_iota(jnp.int32, (s, chunk * s), 1) % s
    allowed = row <= col
    zeros = jnp.zeros((head_dim, chunk * s), BF16)
    pack = 128 // head_dim
    for g in range(n_kv):
        lanes = slice(g // pack * 128, g // pack * 128 + 128)
        k_all = jnp.concatenate([r[0, :, lanes] for r in k_refs], axis=0)
        v_all = jnp.concatenate([r[0, g * head_dim:(g + 1) * head_dim, :] for r in v_refs], axis=1)
        for c in range(groups // chunk):
            h0 = g * groups + c * chunk
            q = jnp.concatenate([q_ref[0, h * head_dim:(h + 1) * head_dim, :] for h in range(h0, h0 + chunk)], axis=1)
            q = jnp.concatenate([q if j == g % pack else zeros for j in range(pack)], axis=0)
            sc = jnp.dot(k_all, q, preferred_element_type=F32)
            full = sc.shape[0] - s
            diag = jnp.where(allowed, sc[full:], -jnp.inf)
            m = jnp.max(diag, axis=0, keepdims=True)
            if full:
                m = jnp.maximum(m, jnp.max(sc[:full], axis=0, keepdims=True))
                sc = jnp.concatenate([sc[:full], diag], axis=0)
            else:
                sc = diag
            e = jnp.exp2((sc - m) * factor)
            l = jnp.sum(e, axis=0, keepdims=True)
            o = jnp.dot(v_all, e.astype(BF16), preferred_element_type=F32) / l
            for h in range(0, chunk, pack):
                stacked = jnp.concatenate([o[:, (h + j) * s:(h + j + 1) * s] for j in range(pack)], axis=0)
                o_ref[0, :, (h0 + h) * head_dim:(h0 + h + pack) * head_dim] = stacked.astype(BF16).T


def attn_body(head_dim, n_kv, chunk, me_ref, q_ref, k0, v0, ka, va, kb, vb, kc, vc, o_ref):
    me = me_ref[0]
    k_sets = {0: [k0], 1: [kc, k0], 2: [ka, kb, k0], 3: [ka, kb, kc, k0]}
    v_sets = {0: [v0], 1: [vc, v0], 2: [va, vb, v0], 3: [va, vb, vc, v0]}
    for d in range(4):
        @pl.when(me == d)
        def _():
            attn_one(head_dim, n_kv, chunk, q_ref, k_sets[d], v_sets[d], o_ref)


def attention(me, q, kvs, head_dim, n_kv, chunk=2):
    n_batch, feats, s = q.shape
    kv = n_kv * head_dim
    flat = [a for pair in kvs for a in pair]
    kspec = pl.BlockSpec((1, s, kv), lambda b, me_ref: (b, 0, 0))
    vspec = pl.BlockSpec((1, kv, s), lambda b, me_ref: (b, 0, 0))
    return pl.pallas_call(
        functools.partial(attn_body, head_dim, n_kv, chunk),
        grid_spec=pltpu.PrefetchScalarGridSpec(
            num_scalar_prefetch=1,
            grid=(n_batch,),
            in_specs=[pl.BlockSpec((1, feats, s), lambda b, me_ref: (b, 0, 0))] + [kspec, vspec] * 4,
            out_specs=pl.BlockSpec((1, s, feats), lambda b, me_ref: (b, 0, 0)),
        ),
        out_shape=jax.ShapeDtypeStruct((n_batch, s, feats), BF16),
        compiler_params=params(),
        cost_estimate=cost(4 * n_batch * feats * s * 256, 4 * n_batch * feats * s),
        name="attention",
    )(me, q, *flat)


def out_body(o_ref, w_ref, x_ref, g_ref, h_ref, r_ref):
    acc = jnp.dot(o_ref[...], w_ref[0], preferred_element_type=F32)
    h = (x_ref[...].astype(F32) + acc).astype(BF16)
    h_ref[...] = h
    r_ref[...] = normed(h, g_ref[0])


def out_proj(layer, o, w, x, gain, tile=256):
    rows, d = x.shape
    k = o.shape[1]
    return pl.pallas_call(
        out_body,
        grid=(rows // tile,),
        in_specs=[
            pl.BlockSpec((tile, k), lambda i: (i, 0)),
            pl.BlockSpec((1, k, d), lambda i: (layer, 0, 0), pipeline_mode=pl.Buffered(1)),
            pl.BlockSpec((tile, d), lambda i: (i, 0)),
            pl.BlockSpec((1, 1, d), lambda i: (layer, 0, 0)),
        ],
        out_specs=[pl.BlockSpec((tile, d), lambda i: (i, 0))] * 2,
        out_shape=[jax.ShapeDtypeStruct((rows, d), BF16)] * 2,
        compiler_params=params(),
        cost_estimate=cost(2 * rows * d * k, 8 * rows * d),
        name="out_proj",
    )(o, w, x, gain)


def mlp_body(n_up, tn, mt, r_ref, wu_ref, wd_ref, h_ref, y_ref, z_ref):
    i = pl.program_id(0)
    rows = r_ref.shape[0]

    @pl.when(i < n_up)
    def _():
        cols = pl.ds(pl.multiple_of(i * tn, tn), tn)
        for m in range(0, rows, mt):
            u = jnp.dot(r_ref[m:m + mt, :], wu_ref[0], preferred_element_type=F32)
            z_ref[m:m + mt, cols] = jax.nn.gelu(u, approximate=True).astype(BF16)

    @pl.when(i >= n_up)
    def _():
        for m in range(0, rows, mt):
            acc = jnp.dot(z_ref[m:m + mt, :], wd_ref[0], preferred_element_type=F32)
            y_ref[m:m + mt, :] = (h_ref[m:m + mt, :].astype(F32) + acc).astype(BF16)


def mlp(layer, r, wu, wd, h, tn=512, td=512, mt=1024):
    rows, d = r.shape
    ff = wu.shape[2]
    n_up = ff // tn
    n_dn = d // td
    return pl.pallas_call(
        functools.partial(mlp_body, n_up, tn, mt),
        grid=(n_up + n_dn,),
        in_specs=[
            pl.BlockSpec((rows, d), lambda i: (0, 0), pipeline_mode=pl.Buffered(1)),
            pl.BlockSpec((1, d, tn), lambda i: (layer, 0, jnp.minimum(i, n_up - 1))),
            pl.BlockSpec((1, ff, td), lambda i: (layer, 0, jnp.maximum(i - n_up, 0))),
            pl.BlockSpec((rows, td), lambda i: (0, jnp.maximum(i - n_up, 0))),
        ],
        out_specs=pl.BlockSpec((rows, td), lambda i: (0, jnp.maximum(i - n_up, 0))),
        out_shape=jax.ShapeDtypeStruct((rows, d), BF16),
        scratch_shapes=[pltpu.VMEM((rows, ff), BF16)],
        compiler_params=params(),
        cost_estimate=cost(4 * rows * d * ff, 4 * ff * d),
        name="mlp",
    )(r, wu, wd, h)


def solution(mesh):
    tok_spec = P(None, ("data", "seq"), None)
    in_specs = (tok_spec, P(("data", "seq"))) + (P(),) * 8

    def device_fn(x_loc, pos_loc, w_query, w_key, w_value, w_out, w_up, w_down, g_attn, g_mlp):
        n_layers, d, n_heads, head_dim = w_query.shape
        n_kv = w_key.shape[2]
        n_batch, s, _ = x_loc.shape
        rows = n_batch * s
        half = head_dim // 2
        inv_freq = ROPE_BASE ** (-jnp.arange(half, dtype=F32) * (2.0 / head_dim))
        angles = inv_freq[:, None] * pos_loc.astype(F32)[None, :]
        cos, sin = jnp.cos(angles), jnp.sin(angles)
        wq = jnp.transpose(w_query, (0, 2, 3, 1)).reshape(n_layers, n_heads * head_dim, d)
        wk = jnp.transpose(w_key, (0, 2, 3, 1)).reshape(n_layers, n_kv * head_dim, d)
        wv = jnp.transpose(w_value, (0, 2, 3, 1)).reshape(n_layers, n_kv * head_dim, d)
        wo = w_out.reshape(n_layers, n_heads * head_dim, d)
        ga = g_attn.reshape(n_layers, 1, d)
        gm = g_mlp.reshape(n_layers, 1, d)
        me = lax.axis_index("seq").astype(jnp.int32).reshape(1)
        x = x_loc.reshape(rows, d)
        for layer in range(n_layers):
            n, k, v = kv_proj(layer, x, ga, wk, wv, cos, sin, head_dim, n_batch)
            cross = [lax.ppermute(a, "seq", ((0, 2), (1, 3))) for a in (k, v)]
            near = [lax.ppermute(a, "seq", ((0, 1), (2, 3))) for a in (k, v)]
            q = q_proj(layer, n, wq, cos, sin, head_dim, n_batch)
            swap = [lax.ppermute(a, "seq", ((2, 3), (3, 2))) for a in cross]
            o = attention(me, q, ((k, v), cross, swap, near), head_dim, n_kv)
            h, r = out_proj(layer, o.reshape(rows, n_heads * head_dim), wo, x, gm)
            x = mlp(layer, r, w_up, w_down, h)
        return x.reshape(x_loc.shape)

    return jax.shard_map(device_fn, mesh=mesh, in_specs=in_specs, out_specs=tok_spec, check_vma=False)
```

```python
import functools

import jax
import jax.numpy as jnp
from jax import lax
from jax.experimental import pallas as pl
from jax.experimental.pallas import tpu as pltpu
from jax.sharding import PartitionSpec as P

ROPE_BASE = 10000.0
NORM_EPS = 1e-6
LOG2E = 1.4426950408889634
F32 = jnp.float32
BF16 = jnp.bfloat16
LANES = 128
NT = (((1,), (1,)), ((), ()))
VMEM_LIMIT = 64 * 1024 * 1024 - 65536


def params(limit=VMEM_LIMIT):
    return pltpu.CompilerParams(dimension_semantics=("arbitrary",), vmem_limit_bytes=limit)


def cost(flops, nbytes):
    return pl.CostEstimate(flops=int(flops), bytes_accessed=int(nbytes), transcendentals=0)


def normed(x_bf16, gain):
    x = x_bf16.astype(F32)
    mean_sq = jnp.mean(x * x, axis=-1, keepdims=True)
    return (x * lax.rsqrt(mean_sq + NORM_EPS) * gain).astype(BF16)


def rope_t(u, cos, sin):
    half = u.shape[0] // 2
    a, b = u[:half], u[half:]
    return jnp.concatenate([a * cos - b * sin, b * cos + a * sin], axis=0).astype(BF16)


def kv_body(head_dim, batch_rows, x_ref, g_ref, wk_ref, wv_ref, cos_ref, sin_ref, n_ref, kv_ref):
    n = normed(x_ref[...], g_ref[0])
    n_ref[...] = n
    k_t = lax.dot_general(wk_ref[0], n, NT, preferred_element_type=F32)
    v_t = lax.dot_general(wv_ref[0], n, NT, preferred_element_type=F32).astype(BF16)
    kv = k_t.shape[0]
    for i in range(n.shape[0] // batch_rows):
        cols = slice(i * batch_rows, (i + 1) * batch_rows)
        heads = [rope_t(k_t[h:h + head_dim, cols], cos_ref[...], sin_ref[...]) for h in range(0, kv, head_dim)]
        per = LANES // head_dim
        for p in range(kv // LANES):
            pair = jnp.concatenate(heads[p * per:(p + 1) * per], axis=0)
            kv_ref[i, p * batch_rows:(p + 1) * batch_rows, :] = pair.T
        kv_ref[i, kv // LANES * batch_rows:, :] = v_t[:, cols]


def kv_proj(layer, x, gain, wk, wv, cos, sin, head_dim, n_batch, tile=256):
    rows, d = x.shape
    kv = wk.shape[1]
    s = rows // n_batch
    per = tile // s
    kv_rows = kv // LANES * s + kv
    return pl.pallas_call(
        functools.partial(kv_body, head_dim, s),
        grid=(rows // tile,),
        in_specs=[
            pl.BlockSpec((tile, d), lambda i: (i, 0)),
            pl.BlockSpec((1, 1, d), lambda i: (layer, 0, 0)),
            pl.BlockSpec((1, kv, d), lambda i: (layer, 0, 0)),
            pl.BlockSpec((1, kv, d), lambda i: (layer, 0, 0)),
            pl.BlockSpec(cos.shape, lambda i: (0, 0)),
            pl.BlockSpec(cos.shape, lambda i: (0, 0)),
        ],
        out_specs=[
            pl.BlockSpec((tile, d), lambda i: (i, 0)),
            pl.BlockSpec((per, kv_rows, s), lambda i: (i, 0, 0)),
        ],
        out_shape=[
            jax.ShapeDtypeStruct((rows, d), BF16),
            jax.ShapeDtypeStruct((n_batch, kv_rows, s), BF16),
        ],
        compiler_params=params(),
        cost_estimate=cost(4 * rows * d * kv, 4 * rows * d),
        name="kv_proj",
    )(x, gain, wk, wv, cos, sin)


def attn_one(head_dim, n_kv, q_ref, b, refs, o_ref):
    s = q_ref.shape[2]
    groups = q_ref.shape[1] // head_dim // n_kv
    factor = LOG2E * head_dim ** -0.5
    pack = LANES // head_dim
    v_row = n_kv // pack * s
    row = lax.broadcasted_iota(jnp.int32, (s, s), 0)
    col = lax.broadcasted_iota(jnp.int32, (s, s), 1)
    allowed = jnp.concatenate([row <= col] * groups, axis=1)
    zeros = jnp.zeros((head_dim, groups * s), BF16)
    for g in range(n_kv):
        k_rows = slice(g // pack * s, (g // pack + 1) * s)
        v_rows = slice(v_row + g * head_dim, v_row + (g + 1) * head_dim)
        k_all = jnp.concatenate([r[b, k_rows, :] for r in refs], axis=0)
        v_all = jnp.concatenate([r[b, v_rows, :] for r in refs], axis=1)
        h0 = g * groups
        q = jnp.concatenate([q_ref[b, h * head_dim:(h + 1) * head_dim, :] for h in range(h0, h0 + groups)], axis=1)
        q = jnp.concatenate([q if j == g % pack else zeros for j in range(pack)], axis=0)
        sc = jnp.dot(k_all, q, preferred_element_type=F32)
        full = sc.shape[0] - s
        diag = jnp.where(allowed, sc[full:], -jnp.inf)
        sc = jnp.concatenate([sc[:full], diag], axis=0) if full else diag
        m = jnp.max(sc, axis=0, keepdims=True)
        e = jnp.exp2((sc - m) * factor)
        l = jnp.sum(e, axis=0, keepdims=True)
        o = jnp.dot(v_all, e.astype(BF16), preferred_element_type=F32) / l
        for h in range(0, groups, pack):
            stacked = jnp.concatenate([o[:, (h + j) * s:(h + j + 1) * s] for j in range(pack)], axis=0)
            o_ref[0, :, (h0 + h) * head_dim:(h0 + h + pack) * head_dim] = stacked.astype(BF16).T


def qattn_body(head_dim, n_kv, nq, fchunk, forward_at, n_ref, wq_ref, cos_ref, sin_ref, own, o_ref,
               q_scr, far, swp, near, s_far, r_far, s_swp, r_swp, s_near, r_near):
    i = pl.program_id(0)
    last = pl.num_programs(0) - 1
    me = lax.axis_index("seq")
    n_batch, feats, s = q_scr.shape
    n_chunks = len(forward_at)
    per = n_batch // n_chunks

    def send(src, dst, sems, rems, c, target):
        if c is None:
            return pltpu.make_async_remote_copy(src_ref=src, dst_ref=dst, send_sem=sems.at[0], recv_sem=rems.at[0],
                                                device_id={"seq": target}, device_id_type=pl.DeviceIdType.MESH)
        rows = pl.ds(c * per, per)
        return pltpu.make_async_remote_copy(src_ref=src.at[rows], dst_ref=dst.at[rows], send_sem=sems.at[c], recv_sem=rems.at[c],
                                            device_id={"seq": target}, device_id_type=pl.DeviceIdType.MESH)

    def far_copy(c):
        return send(own, far, s_far, r_far, c, lax.rem(me + 2, 4))

    def swap_copy(c):
        return send(far, swp, s_swp, r_swp, c, 5 - me)

    def near_copy():
        return send(own, near, s_near, r_near, None, me + 1 - 2 * lax.rem(me, 2))

    @pl.when(i == 0)
    def _():
        barrier = pltpu.get_barrier_semaphore()

        def ready(target):
            pl.semaphore_signal(barrier, inc=1, device_id={"seq": target}, device_id_type=pl.DeviceIdType.MESH)

        @pl.when(me == 0)
        def _():
            pl.semaphore_wait(barrier, 2)

        @pl.when(me == 1)
        def _():
            ready(0)
            pl.semaphore_wait(barrier, 1)

        @pl.when(me == 2)
        def _():
            ready(0)
            ready(3)
            pl.semaphore_wait(barrier, 1)

        @pl.when(me == 3)
        def _():
            ready(1)
            ready(2)
            pl.semaphore_wait(barrier, 1)

        @pl.when(me < 2)
        def _():
            for c in range(n_chunks):
                far_copy(c).start()

        @pl.when(lax.rem(me, 2) == 0)
        def _():
            near_copy().start()

    for c, at in enumerate(forward_at):
        @pl.when((i == at) & (me >= 2))
        def _():
            far_copy(c).wait_recv()
            swap_copy(c).start()

        @pl.when((i == nq + c * per) & (me >= 2))
        def _():
            swap_copy(c).wait_recv()

    @pl.when((i == nq) & (lax.rem(me, 2) == 1))
    def _():
        near_copy().wait_recv()

    @pl.when(i < nq)
    def _():
        for f0 in range(0, feats, fchunk):
            u = lax.dot_general(wq_ref[0, f0:f0 + fchunk, :], n_ref[...], NT, preferred_element_type=F32)
            for j in range(n_ref.shape[0] // s):
                for h in range(0, fchunk, head_dim):
                    q_scr[i * (n_ref.shape[0] // s) + j, f0 + h:f0 + h + head_dim, :] = rope_t(
                        u[h:h + head_dim, j * s:(j + 1) * s], cos_ref[...], sin_ref[...])

    sets = ([own], [near, own], [far, swp, own], [far, swp, near, own])
    for dev, refs in enumerate(sets):
        @pl.when((i >= nq) & (me == dev))
        def _():
            attn_one(head_dim, n_kv, q_scr, i - nq, refs, o_ref)

    @pl.when((i == last) & (me < 2))
    def _():
        for c in range(n_chunks):
            far_copy(c).wait_send()

    @pl.when((i == last) & (me >= 2))
    def _():
        for c in range(n_chunks):
            swap_copy(c).wait_send()

    @pl.when((i == last) & (lax.rem(me, 2) == 0))
    def _():
        near_copy().wait_send()


def q_attention(layer, n, wq, cos, sin, own, head_dim, n_kv, tile=256, fchunk=512):
    rows, d = n.shape
    feats = wq.shape[1]
    n_batch, kv_rows, s = own.shape
    nq = rows // tile
    n_chunks = 8
    forward_at = (3, 5, 7) + tuple(nq + 2 * c + 1 for c in range(n_chunks - 3))
    slot = pltpu.VMEM(own.shape, BF16)
    sems = [pltpu.SemaphoreType.DMA((n_chunks,))] * 4 + [pltpu.SemaphoreType.DMA((1,))] * 2
    return pl.pallas_call(
        functools.partial(qattn_body, head_dim, n_kv, nq, fchunk, forward_at),
        grid=(nq + n_batch,),
        in_specs=[
            pl.BlockSpec((tile, d), lambda i: (jnp.minimum(i, nq - 1), 0)),
            pl.BlockSpec((1, feats, d), lambda i: (layer, 0, 0), pipeline_mode=pl.Buffered(1)),
            pl.BlockSpec(cos.shape, lambda i: (0, 0)),
            pl.BlockSpec(cos.shape, lambda i: (0, 0)),
            pl.BlockSpec(own.shape, lambda i: (0, 0, 0), pipeline_mode=pl.Buffered(1)),
        ],
        out_specs=pl.BlockSpec((1, s, feats), lambda i: (jnp.maximum(i - nq, 0), 0, 0)),
        out_shape=jax.ShapeDtypeStruct((n_batch, s, feats), BF16),
        scratch_shapes=[pltpu.VMEM((n_batch, feats, s), BF16), slot, slot, slot] + sems,
        compiler_params=pltpu.CompilerParams(dimension_semantics=("arbitrary",), vmem_limit_bytes=VMEM_LIMIT,
                                             collective_id=layer, has_side_effects=True),
        cost_estimate=cost(2 * rows * d * feats + 4 * rows * feats * 256, 4 * rows * d + 2 * feats * d),
        name="q_attention",
    )(n, wq, cos, sin, own)


def out_body(o_ref, w_ref, x_ref, g_ref, h_ref, r_ref):
    acc = jnp.dot(o_ref[...], w_ref[0], preferred_element_type=F32)
    h = (x_ref[...].astype(F32) + acc).astype(BF16)
    h_ref[...] = h
    r_ref[...] = normed(h, g_ref[0])


def out_proj(layer, o, w, x, gain, tile=256):
    rows, d = x.shape
    k = o.shape[1]
    return pl.pallas_call(
        out_body,
        grid=(rows // tile,),
        in_specs=[
            pl.BlockSpec((tile, k), lambda i: (i, 0)),
            pl.BlockSpec((1, k, d), lambda i: (layer, 0, 0), pipeline_mode=pl.Buffered(1)),
            pl.BlockSpec((tile, d), lambda i: (i, 0)),
            pl.BlockSpec((1, 1, d), lambda i: (layer, 0, 0)),
        ],
        out_specs=[pl.BlockSpec((tile, d), lambda i: (i, 0))] * 2,
        out_shape=[jax.ShapeDtypeStruct((rows, d), BF16)] * 2,
        compiler_params=params(),
        cost_estimate=cost(2 * rows * d * k, 8 * rows * d),
        name="out_proj",
    )(o, w, x, gain)


def mlp_body(n_up, tn, mt, r_ref, wu_ref, wd_ref, h_ref, y_ref, z_ref):
    i = pl.program_id(0)
    rows = r_ref.shape[0]

    @pl.when(i < n_up)
    def _():
        cols = pl.ds(pl.multiple_of(i * tn, tn), tn)
        for m in range(0, rows, mt):
            u = jnp.dot(r_ref[m:m + mt, :], wu_ref[0], preferred_element_type=F32)
            z_ref[m:m + mt, cols] = jax.nn.gelu(u, approximate=True).astype(BF16)

    @pl.when(i >= n_up)
    def _():
        for m in range(0, rows, mt):
            acc = jnp.dot(z_ref[m:m + mt, :], wd_ref[0], preferred_element_type=F32)
            y_ref[m:m + mt, :] = (h_ref[m:m + mt, :].astype(F32) + acc).astype(BF16)


def mlp(layer, r, wu, wd, h, tn=512, td=512, mt=1024):
    rows, d = r.shape
    ff = wu.shape[2]
    n_up = ff // tn
    n_dn = d // td
    return pl.pallas_call(
        functools.partial(mlp_body, n_up, tn, mt),
        grid=(n_up + n_dn,),
        in_specs=[
            pl.BlockSpec((rows, d), lambda i: (0, 0), pipeline_mode=pl.Buffered(1)),
            pl.BlockSpec((1, d, tn), lambda i: (layer, 0, jnp.minimum(i, n_up - 1))),
            pl.BlockSpec((1, ff, td), lambda i: (layer, 0, jnp.maximum(i - n_up, 0))),
            pl.BlockSpec((rows, td), lambda i: (0, jnp.maximum(i - n_up, 0))),
        ],
        out_specs=pl.BlockSpec((rows, td), lambda i: (0, jnp.maximum(i - n_up, 0))),
        out_shape=jax.ShapeDtypeStruct((rows, d), BF16),
        scratch_shapes=[pltpu.VMEM((rows, ff), BF16)],
        compiler_params=params(),
        cost_estimate=cost(4 * rows * d * ff, 4 * ff * d),
        name="mlp",
    )(r, wu, wd, h)


def solution(mesh):
    tok_spec = P(None, ("data", "seq"), None)
    in_specs = (tok_spec, P(("data", "seq"))) + (P(),) * 8

    def device_fn(x_loc, pos_loc, w_query, w_key, w_value, w_out, w_up, w_down, g_attn, g_mlp):
        n_layers, d, n_heads, head_dim = w_query.shape
        n_kv = w_key.shape[2]
        n_batch, s, _ = x_loc.shape
        rows = n_batch * s
        half = head_dim // 2
        inv_freq = ROPE_BASE ** (-jnp.arange(half, dtype=F32) * (2.0 / head_dim))
        angles = inv_freq[:, None] * pos_loc.astype(F32)[None, :]
        cos, sin = jnp.cos(angles), jnp.sin(angles)
        wq = jnp.transpose(w_query, (0, 2, 3, 1)).reshape(n_layers, n_heads * head_dim, d)
        wk = jnp.transpose(w_key, (0, 2, 3, 1)).reshape(n_layers, n_kv * head_dim, d)
        wv = jnp.transpose(w_value, (0, 2, 3, 1)).reshape(n_layers, n_kv * head_dim, d)
        wo = w_out.reshape(n_layers, n_heads * head_dim, d)
        ga = g_attn.reshape(n_layers, 1, d)
        gm = g_mlp.reshape(n_layers, 1, d)
        x = x_loc.reshape(rows, d)
        for layer in range(n_layers):
            n, kv = kv_proj(layer, x, ga, wk, wv, cos, sin, head_dim, n_batch)
            o = q_attention(layer, n, wq, cos, sin, kv, head_dim, n_kv)
            h, r = out_proj(layer, o.reshape(rows, n_heads * head_dim), wo, x, gm)
            x = mlp(layer, r, w_up, w_down, h)
        return x.reshape(x_loc.shape)

    return jax.shard_map(device_fn, mesh=mesh, in_specs=in_specs, out_specs=tok_spec, check_vma=False)
```

```python
import functools
import math

import jax
import jax.numpy as jnp
from jax import lax
from jax.experimental import pallas as pl
from jax.experimental.pallas import tpu as pltpu
from jax.sharding import PartitionSpec as P

ROPE_BASE = 10000.0
NORM_EPS = 1e-6
LOG2E = 1.4426950408889634
F32 = jnp.float32
BF16 = jnp.bfloat16
LANES = 128
NT = (((1,), (1,)), ((), ()))
VMEM_LIMIT = 64 * 1024 * 1024 - 65536


def params(limit=VMEM_LIMIT):
    return pltpu.CompilerParams(dimension_semantics=("arbitrary",), vmem_limit_bytes=limit)


def cost(flops, nbytes):
    return pl.CostEstimate(flops=int(flops), bytes_accessed=int(nbytes), transcendentals=0)


def normed(x_bf16, gain):
    x = x_bf16.astype(F32)
    mean_sq = jnp.mean(x * x, axis=-1, keepdims=True)
    return (x * lax.rsqrt(mean_sq + NORM_EPS) * gain).astype(BF16)


def rope_t(u, cos, sin):
    half = u.shape[0] // 2
    a, b = u[:half], u[half:]
    return jnp.concatenate([a * cos - b * sin, b * cos + a * sin], axis=0).astype(BF16)


def kv_body(head_dim, batch_rows, x_ref, g_ref, wk_ref, wv_ref, cos_ref, sin_ref, n_ref, kv_ref):
    n = normed(x_ref[...], g_ref[0])
    n_ref[...] = n
    k_t = lax.dot_general(wk_ref[0], n, NT, preferred_element_type=F32)
    v_t = lax.dot_general(wv_ref[0], n, NT, preferred_element_type=F32).astype(BF16)
    kv = k_t.shape[0]
    for i in range(n.shape[0] // batch_rows):
        cols = slice(i * batch_rows, (i + 1) * batch_rows)
        heads = [rope_t(k_t[h:h + head_dim, cols], cos_ref[...], sin_ref[...]) for h in range(0, kv, head_dim)]
        per = LANES // head_dim
        for p in range(kv // LANES):
            pair = jnp.concatenate(heads[p * per:(p + 1) * per], axis=0)
            kv_ref[i, p * batch_rows:(p + 1) * batch_rows, :] = pair.T
        kv_ref[i, kv // LANES * batch_rows:, :] = v_t[:, cols]


def kv_proj(layer, x, gain, wk, wv, cos, sin, head_dim, n_batch, tile=512):
    rows, d = x.shape
    kv = wk.shape[1]
    s = rows // n_batch
    per = tile // s
    kv_rows = kv // LANES * s + kv
    return pl.pallas_call(
        functools.partial(kv_body, head_dim, s),
        grid=(rows // tile,),
        in_specs=[
            pl.BlockSpec((tile, d), lambda i: (i, 0)),
            pl.BlockSpec((1, 1, d), lambda i: (layer, 0, 0)),
            pl.BlockSpec((1, kv, d), lambda i: (layer, 0, 0)),
            pl.BlockSpec((1, kv, d), lambda i: (layer, 0, 0)),
            pl.BlockSpec(cos.shape, lambda i: (0, 0)),
            pl.BlockSpec(cos.shape, lambda i: (0, 0)),
        ],
        out_specs=[
            pl.BlockSpec((tile, d), lambda i: (i, 0)),
            pl.BlockSpec((per, kv_rows, s), lambda i: (i, 0, 0)),
        ],
        out_shape=[
            jax.ShapeDtypeStruct((rows, d), BF16),
            jax.ShapeDtypeStruct((n_batch, kv_rows, s), BF16),
        ],
        compiler_params=params(),
        cost_estimate=cost(4 * rows * d * kv, 4 * rows * d),
        name="kv_proj",
    )(x, gain, wk, wv, cos, sin)


def scores(head_dim, n_kv, g, q_ref, b, refs, sc_ref, m_ref):
    s = q_ref.shape[2]
    groups = q_ref.shape[1] // head_dim // n_kv
    pack = LANES // head_dim
    k_rows = slice(g // pack * s, (g // pack + 1) * s)
    k_all = jnp.concatenate([r[b, k_rows, :] for r in refs], axis=0)
    h0 = g * groups
    q = jnp.concatenate([q_ref[b, h * head_dim:(h + 1) * head_dim, :] for h in range(h0, h0 + groups)], axis=1)
    zeros = jnp.zeros(q.shape, BF16)
    q = jnp.concatenate([q if j == g % pack else zeros for j in range(pack)], axis=0)
    sc = jnp.dot(k_all, q, preferred_element_type=F32)
    row = lax.broadcasted_iota(jnp.int32, (s, s), 0)
    col = lax.broadcasted_iota(jnp.int32, (s, s), 1)
    allowed = jnp.concatenate([row <= col] * groups, axis=1)
    full = sc.shape[0] - s
    diag = jnp.where(allowed, sc[full:], -jnp.inf)
    sc = jnp.concatenate([sc[:full], diag], axis=0) if full else diag
    sc_ref[:full + s, :] = sc
    m_ref[...] = jnp.broadcast_to(jnp.max(sc, axis=0, keepdims=True), m_ref.shape)


def combine(head_dim, n_kv, g, b, refs, sc_ref, m_ref, o_ref):
    s = o_ref.shape[1]
    groups = o_ref.shape[2] // head_dim // n_kv
    pack = LANES // head_dim
    v_row = n_kv // pack * s + g * head_dim
    v_all = jnp.concatenate([r[b, v_row:v_row + head_dim, :] for r in refs], axis=1)
    e = jnp.exp2((sc_ref[:len(refs) * s, :] - m_ref[0:1, :]) * (LOG2E * head_dim ** -0.5))
    l = jnp.sum(e, axis=0, keepdims=True)
    o = jnp.dot(v_all, e.astype(BF16), preferred_element_type=F32) / l
    for h in range(0, groups, pack):
        stacked = jnp.concatenate([o[:, (h + j) * s:(h + j + 1) * s] for j in range(pack)], axis=0)
        lane = (g * groups + h) * head_dim
        o_ref[0, :, lane:lane + LANES] = stacked.astype(BF16).T


def qattn_body(head_dim, n_kv, nq, fchunk, forward_at, n_ref, wq_ref, cos_ref, sin_ref, own, o_ref,
               q_scr, sc_a, sc_b, m_a, m_b, far, swp, near, s_far, r_far, s_swp, r_swp, s_near, r_near):
    i = pl.program_id(0)
    last = pl.num_programs(0) - 1
    me = lax.axis_index("seq")
    n_batch, feats, s = q_scr.shape
    n_chunks = len(forward_at)
    per = n_batch // n_chunks

    def send(src, dst, sems, rems, c, target):
        if c is None:
            return pltpu.make_async_remote_copy(src_ref=src, dst_ref=dst, send_sem=sems.at[0], recv_sem=rems.at[0],
                                                device_id={"seq": target}, device_id_type=pl.DeviceIdType.MESH)
        rows = pl.ds(c * per, per)
        return pltpu.make_async_remote_copy(src_ref=src.at[rows], dst_ref=dst.at[rows], send_sem=sems.at[c], recv_sem=rems.at[c],
                                            device_id={"seq": target}, device_id_type=pl.DeviceIdType.MESH)

    def far_copy(c):
        return send(own, far, s_far, r_far, c, lax.rem(me + 2, 4))

    def swap_copy(c):
        return send(far, swp, s_swp, r_swp, c, 5 - me)

    def near_copy():
        return send(own, near, s_near, r_near, None, me + 1 - 2 * lax.rem(me, 2))

    @pl.when(i == 0)
    def _():
        barrier = pltpu.get_barrier_semaphore()

        def ready(target):
            pl.semaphore_signal(barrier, inc=1, device_id={"seq": target}, device_id_type=pl.DeviceIdType.MESH)

        @pl.when(me == 0)
        def _():
            pl.semaphore_wait(barrier, 2)

        @pl.when(me == 1)
        def _():
            ready(0)
            pl.semaphore_wait(barrier, 1)

        @pl.when(me == 2)
        def _():
            ready(0)
            ready(3)
            pl.semaphore_wait(barrier, 1)

        @pl.when(me == 3)
        def _():
            ready(1)
            ready(2)
            pl.semaphore_wait(barrier, 1)

        @pl.when(me < 2)
        def _():
            for c in range(n_chunks):
                far_copy(c).start()

        @pl.when(lax.rem(me, 2) == 0)
        def _():
            near_copy().start()

    for c, at in enumerate(forward_at):
        @pl.when((i == at) & (me >= 2))
        def _():
            far_copy(c).wait_recv()
            swap_copy(c).start()

        @pl.when((i == nq + max(c * per - 1, 0)) & (me >= 2))
        def _():
            swap_copy(c).wait_recv()

    @pl.when((i == nq) & (lax.rem(me, 2) == 1))
    def _():
        near_copy().wait_recv()

    @pl.when(i < nq)
    def _():
        for f0 in range(0, feats, fchunk):
            u = lax.dot_general(wq_ref[0, f0:f0 + fchunk, :], n_ref[...], NT, preferred_element_type=F32)
            for j in range(n_ref.shape[0] // s):
                for h in range(0, fchunk, head_dim):
                    q_scr[i * (n_ref.shape[0] // s) + j, f0 + h:f0 + h + head_dim, :] = rope_t(
                        u[h:h + head_dim, j * s:(j + 1) * s], cos_ref[...], sin_ref[...])

    sets = ([own], [near, own], [far, swp, own], [far, swp, near, own])
    b = jnp.maximum(i - nq, 0)
    after = jnp.minimum(b + 1, n_batch - 1)
    bufs = ((sc_a, m_a), (sc_b, m_b))
    for dev, refs in enumerate(sets):
        @pl.when((i == nq) & (me == dev))
        def _():
            scores(head_dim, n_kv, 0, q_scr, 0, refs, *bufs[0])

        for g in range(n_kv):
            @pl.when((i >= nq) & (me == dev))
            def _():
                scores(head_dim, n_kv, (g + 1) % n_kv, q_scr, b if g + 1 < n_kv else after, refs, *bufs[(g + 1) % 2])
                combine(head_dim, n_kv, g, b, refs, *bufs[g % 2], o_ref)

    @pl.when((i == last) & (me < 2))
    def _():
        for c in range(n_chunks):
            far_copy(c).wait_send()

    @pl.when((i == last) & (me >= 2))
    def _():
        for c in range(n_chunks):
            swap_copy(c).wait_send()

    @pl.when((i == last) & (lax.rem(me, 2) == 0))
    def _():
        near_copy().wait_send()


def q_attention(layer, n, wq, cos, sin, own, head_dim, n_kv, tile=256, fchunk=512):
    rows, d = n.shape
    feats = wq.shape[1]
    n_batch, kv_rows, s = own.shape
    nq = rows // tile
    n_chunks = 8
    forward_at = (3, 5, 7) + tuple(nq + 2 * c + 1 for c in range(n_chunks - 3))
    slot = pltpu.VMEM(own.shape, BF16)
    wide = feats // head_dim // n_kv * s
    soft = [pltpu.VMEM((4 * s, wide), F32)] * 2 + [pltpu.VMEM((8, wide), F32)] * 2
    sems = [pltpu.SemaphoreType.DMA((n_chunks,))] * 4 + [pltpu.SemaphoreType.DMA((1,))] * 2
    return pl.pallas_call(
        functools.partial(qattn_body, head_dim, n_kv, nq, fchunk, forward_at),
        grid=(nq + n_batch,),
        in_specs=[
            pl.BlockSpec((tile, d), lambda i: (jnp.minimum(i, nq - 1), 0)),
            pl.BlockSpec((1, feats, d), lambda i: (layer, 0, 0), pipeline_mode=pl.Buffered(1)),
            pl.BlockSpec(cos.shape, lambda i: (0, 0)),
            pl.BlockSpec(cos.shape, lambda i: (0, 0)),
            pl.BlockSpec(own.shape, lambda i: (0, 0, 0), pipeline_mode=pl.Buffered(1)),
        ],
        out_specs=pl.BlockSpec((1, s, feats), lambda i: (jnp.maximum(i - nq, 0), 0, 0)),
        out_shape=jax.ShapeDtypeStruct((n_batch, s, feats), BF16),
        scratch_shapes=[pltpu.VMEM((n_batch, feats, s), BF16)] + soft + [slot, slot, slot] + sems,
        compiler_params=pltpu.CompilerParams(dimension_semantics=("arbitrary",), vmem_limit_bytes=VMEM_LIMIT,
                                             collective_id=layer, has_side_effects=True),
        cost_estimate=cost(2 * rows * d * feats + 4 * rows * feats * 256, 4 * rows * d + 2 * feats * d),
        name="q_attention",
    )(n, wq, cos, sin, own)


def out_body(o_ref, w_ref, x_ref, g_ref, h_ref, r_ref):
    acc = jnp.dot(o_ref[...], w_ref[0], preferred_element_type=F32)
    h = (x_ref[...].astype(F32) + acc).astype(BF16)
    h_ref[...] = h
    r_ref[...] = normed(h, g_ref[0])


def out_proj(layer, o, w, x, gain, tile=256):
    rows, d = x.shape
    k = o.shape[1]
    return pl.pallas_call(
        out_body,
        grid=(rows // tile,),
        in_specs=[
            pl.BlockSpec((tile, k), lambda i: (i, 0)),
            pl.BlockSpec((1, k, d), lambda i: (layer, 0, 0), pipeline_mode=pl.Buffered(1)),
            pl.BlockSpec((tile, d), lambda i: (i, 0)),
            pl.BlockSpec((1, 1, d), lambda i: (layer, 0, 0)),
        ],
        out_specs=[pl.BlockSpec((tile, d), lambda i: (i, 0))] * 2,
        out_shape=[jax.ShapeDtypeStruct((rows, d), BF16)] * 2,
        compiler_params=params(),
        cost_estimate=cost(2 * rows * d * k, 8 * rows * d),
        name="out_proj",
    )(o, w, x, gain)


def gelu_tanh(x):
    root = (2.0 / math.pi) ** 0.5
    half = 0.5 * x
    return half + half * jnp.tanh(x * (root + (root * 0.044715) * (x * x)))


def mlp_body(n_up, tn, mt, r_ref, wu_ref, wd_ref, h_ref, y_ref, z_ref):
    i = pl.program_id(0)
    rows = r_ref.shape[0]

    @pl.when(i < n_up)
    def _():
        cols = pl.ds(pl.multiple_of(i * tn, tn), tn)
        for m in range(0, rows, mt):
            u = jnp.dot(r_ref[m:m + mt, :], wu_ref[0], preferred_element_type=F32)
            z_ref[m:m + mt, cols] = gelu_tanh(u).astype(BF16)

    @pl.when(i >= n_up)
    def _():
        for m in range(0, rows, mt):
            acc = jnp.dot(z_ref[m:m + mt, :], wd_ref[0], preferred_element_type=F32)
            y_ref[m:m + mt, :] = (h_ref[m:m + mt, :].astype(F32) + acc).astype(BF16)


def mlp(layer, r, wu, wd, h, tn=512, td=256, mt=1024):
    rows, d = r.shape
    ff = wu.shape[2]
    n_up = ff // tn
    n_dn = d // td
    return pl.pallas_call(
        functools.partial(mlp_body, n_up, tn, mt),
        grid=(n_up + n_dn,),
        in_specs=[
            pl.BlockSpec((rows, d), lambda i: (0, 0), pipeline_mode=pl.Buffered(1)),
            pl.BlockSpec((1, d, tn), lambda i: (layer, 0, jnp.minimum(i, n_up - 1))),
            pl.BlockSpec((1, ff, td), lambda i: (layer, 0, jnp.maximum(i - n_up, 0))),
            pl.BlockSpec((rows, td), lambda i: (0, jnp.maximum(i - n_up, 0))),
        ],
        out_specs=pl.BlockSpec((rows, td), lambda i: (0, jnp.maximum(i - n_up, 0))),
        out_shape=jax.ShapeDtypeStruct((rows, d), BF16),
        scratch_shapes=[pltpu.VMEM((rows, ff), BF16)],
        compiler_params=params(),
        cost_estimate=cost(4 * rows * d * ff, 4 * ff * d),
        name="mlp",
    )(r, wu, wd, h)


def solution(mesh):
    tok_spec = P(None, ("data", "seq"), None)
    in_specs = (tok_spec, P(("data", "seq"))) + (P(),) * 8

    def device_fn(x_loc, pos_loc, w_query, w_key, w_value, w_out, w_up, w_down, g_attn, g_mlp):
        n_layers, d, n_heads, head_dim = w_query.shape
        n_kv = w_key.shape[2]
        n_batch, s, _ = x_loc.shape
        rows = n_batch * s
        half = head_dim // 2
        inv_freq = ROPE_BASE ** (-jnp.arange(half, dtype=F32) * (2.0 / head_dim))
        angles = inv_freq[:, None] * pos_loc.astype(F32)[None, :]
        cos, sin = jnp.cos(angles), jnp.sin(angles)
        wq = jnp.transpose(w_query, (0, 2, 3, 1)).reshape(n_layers, n_heads * head_dim, d)
        wk = jnp.transpose(w_key, (0, 2, 3, 1)).reshape(n_layers, n_kv * head_dim, d)
        wv = jnp.transpose(w_value, (0, 2, 3, 1)).reshape(n_layers, n_kv * head_dim, d)
        wo = w_out.reshape(n_layers, n_heads * head_dim, d)
        ga = g_attn.reshape(n_layers, 1, d)
        gm = g_mlp.reshape(n_layers, 1, d)
        x = x_loc.reshape(rows, d)
        for layer in range(n_layers):
            n, kv = kv_proj(layer, x, ga, wk, wv, cos, sin, head_dim, n_batch)
            o = q_attention(layer, n, wq, cos, sin, kv, head_dim, n_kv)
            h, r = out_proj(layer, o.reshape(rows, n_heads * head_dim), wo, x, gm)
            x = mlp(layer, r, w_up, w_down, h)
        return x.reshape(x_loc.shape)

    return jax.shard_map(device_fn, mesh=mesh, in_specs=in_specs, out_specs=tok_spec, check_vma=False)
```

```python
import functools
import math

import jax
import jax.numpy as jnp
from jax import lax
from jax.experimental import pallas as pl
from jax.experimental.pallas import tpu as pltpu
from jax.sharding import PartitionSpec as P

ROPE_BASE = 10000.0
NORM_EPS = 1e-6
LOG2E = 1.4426950408889634
F32 = jnp.float32
BF16 = jnp.bfloat16
LANES = 128
NT = (((1,), (1,)), ((), ()))
VMEM_LIMIT = 64 * 1024 * 1024 - 65536


def params(limit=VMEM_LIMIT):
    return pltpu.CompilerParams(dimension_semantics=("arbitrary",), vmem_limit_bytes=limit)


def cost(flops, nbytes):
    return pl.CostEstimate(flops=int(flops), bytes_accessed=int(nbytes), transcendentals=0)


def normed(x_bf16, gain):
    x = x_bf16.astype(F32)
    mean_sq = jnp.mean(x * x, axis=-1, keepdims=True)
    return (x * lax.rsqrt(mean_sq + NORM_EPS) * gain).astype(BF16)


def rope_t(u, cos, sin):
    half = u.shape[0] // 2
    a, b = u[:half], u[half:]
    return jnp.concatenate([a * cos - b * sin, b * cos + a * sin], axis=0).astype(BF16)


def kv_body(layer, head_dim, batch_rows, x_ref, g_ref, wk_ref, wv_ref, cos_ref, sin_ref, n_ref, kv_ref):
    n = normed(x_ref[...], g_ref[layer:layer + 1, :])
    n_ref[...] = n
    k_t = lax.dot_general(wk_ref[0], n, NT, preferred_element_type=F32)
    v_t = lax.dot_general(wv_ref[0], n, NT, preferred_element_type=F32).astype(BF16)
    kv = k_t.shape[0]
    for i in range(n.shape[0] // batch_rows):
        cols = slice(i * batch_rows, (i + 1) * batch_rows)
        heads = [rope_t(k_t[h:h + head_dim, cols], cos_ref[...], sin_ref[...]) for h in range(0, kv, head_dim)]
        per = LANES // head_dim
        for p in range(kv // LANES):
            pair = jnp.concatenate(heads[p * per:(p + 1) * per], axis=0)
            kv_ref[i, p * batch_rows:(p + 1) * batch_rows, :] = pair.T
        kv_ref[i, kv // LANES * batch_rows:, :] = v_t[:, cols]


def kv_proj(layer, x, gain, wk, wv, cos, sin, head_dim, n_batch, tile=512):
    rows, d = x.shape
    kv = wk.shape[1]
    s = rows // n_batch
    per = tile // s
    kv_rows = kv // LANES * s + kv
    return pl.pallas_call(
        functools.partial(kv_body, layer, head_dim, s),
        grid=(rows // tile,),
        in_specs=[
            pl.BlockSpec((tile, d), lambda i: (i, 0)),
            pl.BlockSpec(gain.shape, lambda i: (0, 0)),
            pl.BlockSpec((1, kv, d), lambda i: (layer, 0, 0)),
            pl.BlockSpec((1, kv, d), lambda i: (layer, 0, 0)),
            pl.BlockSpec(cos.shape, lambda i: (0, 0)),
            pl.BlockSpec(cos.shape, lambda i: (0, 0)),
        ],
        out_specs=[
            pl.BlockSpec((tile, d), lambda i: (i, 0)),
            pl.BlockSpec((per, kv_rows, s), lambda i: (i, 0, 0)),
        ],
        out_shape=[
            jax.ShapeDtypeStruct((rows, d), BF16),
            jax.ShapeDtypeStruct((n_batch, kv_rows, s), BF16),
        ],
        compiler_params=params(),
        cost_estimate=cost(4 * rows * d * kv, 4 * rows * d),
        name="kv_proj",
    )(x, gain, wk, wv, cos, sin)


def scores(head_dim, n_kv, g, q_ref, b, refs, sc_ref, m_ref):
    s = q_ref.shape[2]
    groups = q_ref.shape[1] // head_dim // n_kv
    pack = LANES // head_dim
    k_rows = slice(g // pack * s, (g // pack + 1) * s)
    k_all = jnp.concatenate([r[b, k_rows, :] for r in refs], axis=0)
    h0 = g * groups
    q = jnp.concatenate([q_ref[b, h * head_dim:(h + 1) * head_dim, :] for h in range(h0, h0 + groups)], axis=1)
    zeros = jnp.zeros(q.shape, BF16)
    q = jnp.concatenate([q if j == g % pack else zeros for j in range(pack)], axis=0)
    sc = jnp.dot(k_all, q, preferred_element_type=F32)
    row = lax.broadcasted_iota(jnp.int32, (s, s), 0)
    col = lax.broadcasted_iota(jnp.int32, (s, s), 1)
    allowed = jnp.concatenate([row <= col] * groups, axis=1)
    full = sc.shape[0] - s
    diag = jnp.where(allowed, sc[full:], -jnp.inf)
    sc = jnp.concatenate([sc[:full], diag], axis=0) if full else diag
    sc_ref[:full + s, :] = sc
    m_ref[...] = jnp.broadcast_to(jnp.max(sc, axis=0, keepdims=True), m_ref.shape)


def combine(head_dim, n_kv, g, b, refs, sc_ref, m_ref, o_ref):
    s = o_ref.shape[1]
    groups = o_ref.shape[2] // head_dim // n_kv
    pack = LANES // head_dim
    v_row = n_kv // pack * s + g * head_dim
    v_all = jnp.concatenate([r[b, v_row:v_row + head_dim, :] for r in refs], axis=1)
    e = jnp.exp2((sc_ref[:len(refs) * s, :] - m_ref[0:1, :]) * (LOG2E * head_dim ** -0.5))
    l = jnp.sum(e, axis=0, keepdims=True)
    o = jnp.dot(v_all, e.astype(BF16), preferred_element_type=F32) / l
    for h in range(0, groups, pack):
        stacked = jnp.concatenate([o[:, (h + j) * s:(h + j + 1) * s] for j in range(pack)], axis=0)
        lane = (g * groups + h) * head_dim
        o_ref[0, :, lane:lane + LANES] = stacked.astype(BF16).T


def qattn_body(layer, head_dim, n_kv, nq, fchunk, forward_at, n_ref, wq_ref, cos_ref, sin_ref, own, o_ref,
               q_scr, w_scr, w_sem, sc_a, sc_b, m_a, m_b, far, swp, near, s_far, r_far, s_swp, r_swp, s_near, r_near):
    i = pl.program_id(0)
    last = pl.num_programs(0) - 1
    me = lax.axis_index("seq")
    n_batch, feats, s = q_scr.shape
    n_chunks = len(forward_at)
    per = n_batch // n_chunks

    def send(src, dst, sems, rems, c, target):
        if c is None:
            return pltpu.make_async_remote_copy(src_ref=src, dst_ref=dst, send_sem=sems.at[0], recv_sem=rems.at[0],
                                                device_id={"seq": target}, device_id_type=pl.DeviceIdType.MESH)
        rows = pl.ds(c * per, per)
        return pltpu.make_async_remote_copy(src_ref=src.at[rows], dst_ref=dst.at[rows], send_sem=sems.at[c], recv_sem=rems.at[c],
                                            device_id={"seq": target}, device_id_type=pl.DeviceIdType.MESH)

    def far_copy(c):
        return send(own, far, s_far, r_far, c, lax.rem(me + 2, 4))

    def swap_copy(c):
        return send(far, swp, s_swp, r_swp, c, 5 - me)

    def near_copy():
        return send(own, near, s_near, r_near, None, me + 1 - 2 * lax.rem(me, 2))

    def weight_copy(c):
        part = slice(c * fchunk, (c + 1) * fchunk)
        return pltpu.make_async_copy(wq_ref.at[layer, part, :], w_scr.at[part, :], w_sem.at[c])

    @pl.when(i == 0)
    def _():
        for c in range(feats // fchunk):
            weight_copy(c).start()
        barrier = pltpu.get_barrier_semaphore()

        def ready(target):
            pl.semaphore_signal(barrier, inc=1, device_id={"seq": target}, device_id_type=pl.DeviceIdType.MESH)

        @pl.when(me == 0)
        def _():
            pl.semaphore_wait(barrier, 2)

        @pl.when(me == 1)
        def _():
            ready(0)
            pl.semaphore_wait(barrier, 1)

        @pl.when(me == 2)
        def _():
            ready(0)
            ready(3)
            pl.semaphore_wait(barrier, 1)

        @pl.when(me == 3)
        def _():
            ready(1)
            ready(2)
            pl.semaphore_wait(barrier, 1)

        @pl.when(me < 2)
        def _():
            for c in range(n_chunks):
                far_copy(c).start()

        @pl.when(lax.rem(me, 2) == 0)
        def _():
            near_copy().start()

    for c, at in enumerate(forward_at):
        @pl.when((i == at) & (me >= 2))
        def _():
            far_copy(c).wait_recv()
            swap_copy(c).start()

        @pl.when((i == nq + max(c * per - 1, 0)) & (me >= 2))
        def _():
            swap_copy(c).wait_recv()

    @pl.when((i == nq) & (lax.rem(me, 2) == 1))
    def _():
        near_copy().wait_recv()

    def project(f0):
        u = lax.dot_general(w_scr[f0:f0 + fchunk, :], n_ref[...], NT, preferred_element_type=F32)
        for j in range(n_ref.shape[0] // s):
            for h in range(0, fchunk, head_dim):
                q_scr[i * (n_ref.shape[0] // s) + j, f0 + h:f0 + h + head_dim, :] = rope_t(
                    u[h:h + head_dim, j * s:(j + 1) * s], cos_ref[...], sin_ref[...])

    @pl.when(i == 0)
    def _():
        for c, f0 in enumerate(range(0, feats, fchunk)):
            weight_copy(c).wait()
            project(f0)

    @pl.when((i > 0) & (i < nq))
    def _():
        for f0 in range(0, feats, fchunk):
            project(f0)

    sets = ([own], [near, own], [far, swp, own], [far, swp, near, own])
    b = jnp.maximum(i - nq, 0)
    after = jnp.minimum(b + 1, n_batch - 1)
    bufs = ((sc_a, m_a), (sc_b, m_b))
    for dev, refs in enumerate(sets):
        @pl.when((i == nq) & (me == dev))
        def _():
            scores(head_dim, n_kv, 0, q_scr, 0, refs, *bufs[0])

        for g in range(n_kv):
            @pl.when((i >= nq) & (me == dev))
            def _():
                scores(head_dim, n_kv, (g + 1) % n_kv, q_scr, b if g + 1 < n_kv else after, refs, *bufs[(g + 1) % 2])
                combine(head_dim, n_kv, g, b, refs, *bufs[g % 2], o_ref)

    @pl.when((i == last) & (me < 2))
    def _():
        for c in range(n_chunks):
            far_copy(c).wait_send()

    @pl.when((i == last) & (me >= 2))
    def _():
        for c in range(n_chunks):
            swap_copy(c).wait_send()

    @pl.when((i == last) & (lax.rem(me, 2) == 0))
    def _():
        near_copy().wait_send()


def q_attention(layer, n, wq, cos, sin, own, head_dim, n_kv, tile=256, fchunk=512):
    rows, d = n.shape
    feats = wq.shape[1]
    n_batch, kv_rows, s = own.shape
    nq = rows // tile
    n_chunks = 8
    forward_at = (3, 5, 7) + tuple(nq + 2 * c + 1 for c in range(n_chunks - 3))
    slot = pltpu.VMEM(own.shape, BF16)
    wide = feats // head_dim // n_kv * s
    soft = [pltpu.VMEM((4 * s, wide), F32)] * 2 + [pltpu.VMEM((8, wide), F32)] * 2
    sems = [pltpu.SemaphoreType.DMA((n_chunks,))] * 4 + [pltpu.SemaphoreType.DMA((1,))] * 2
    return pl.pallas_call(
        functools.partial(qattn_body, layer, head_dim, n_kv, nq, fchunk, forward_at),
        grid=(nq + n_batch,),
        in_specs=[
            pl.BlockSpec((tile, d), lambda i: (jnp.minimum(i, nq - 1), 0)),
            pl.BlockSpec(memory_space=pl.ANY),
            pl.BlockSpec(cos.shape, lambda i: (0, 0)),
            pl.BlockSpec(cos.shape, lambda i: (0, 0)),
            pl.BlockSpec(own.shape, lambda i: (0, 0, 0), pipeline_mode=pl.Buffered(1)),
        ],
        out_specs=pl.BlockSpec((1, s, feats), lambda i: (jnp.maximum(i - nq, 0), 0, 0)),
        out_shape=jax.ShapeDtypeStruct((n_batch, s, feats), BF16),
        scratch_shapes=[pltpu.VMEM((n_batch, feats, s), BF16), pltpu.VMEM((feats, d), BF16),
                        pltpu.SemaphoreType.DMA((feats // fchunk,))] + soft + [slot, slot, slot] + sems,
        compiler_params=pltpu.CompilerParams(dimension_semantics=("arbitrary",), vmem_limit_bytes=VMEM_LIMIT,
                                             collective_id=layer, has_side_effects=True),
        cost_estimate=cost(2 * rows * d * feats + 4 * rows * feats * 256, 4 * rows * d + 2 * feats * d),
        name="q_attention",
    )(n, wq, cos, sin, own)


def out_body(layer, o_ref, w_ref, x_ref, g_ref, h_ref, r_ref):
    acc = jnp.dot(o_ref[...], w_ref[0], preferred_element_type=F32)
    h = (x_ref[...].astype(F32) + acc).astype(BF16)
    h_ref[...] = h
    r_ref[...] = normed(h, g_ref[layer:layer + 1, :])


def out_proj(layer, o, w, x, gain, tile=256):
    rows, d = x.shape
    k = o.shape[1]
    return pl.pallas_call(
        functools.partial(out_body, layer),
        grid=(rows // tile,),
        in_specs=[
            pl.BlockSpec((tile, k), lambda i: (i, 0)),
            pl.BlockSpec((1, k, d), lambda i: (layer, 0, 0), pipeline_mode=pl.Buffered(1)),
            pl.BlockSpec((tile, d), lambda i: (i, 0)),
            pl.BlockSpec(gain.shape, lambda i: (0, 0)),
        ],
        out_specs=[pl.BlockSpec((tile, d), lambda i: (i, 0))] * 2,
        out_shape=[jax.ShapeDtypeStruct((rows, d), BF16)] * 2,
        compiler_params=params(),
        cost_estimate=cost(2 * rows * d * k, 8 * rows * d),
        name="out_proj",
    )(o, w, x, gain)


def gelu_tanh(x):
    root = (2.0 / math.pi) ** 0.5
    half = 0.5 * x
    return half + half * jnp.tanh(x * (root + (root * 0.044715) * (x * x)))


def mlp_body(n_up, tn, mt, r_ref, wu_ref, wd_ref, h_ref, y_ref, z_ref):
    i = pl.program_id(0)
    rows = r_ref.shape[0]

    @pl.when(i < n_up)
    def _():
        cols = pl.ds(pl.multiple_of(i * tn, tn), tn)
        for m in range(0, rows, mt):
            u = jnp.dot(r_ref[m:m + mt, :], wu_ref[0], preferred_element_type=F32)
            z_ref[m:m + mt, cols] = gelu_tanh(u).astype(BF16)

    @pl.when(i >= n_up)
    def _():
        for m in range(0, rows, mt):
            acc = jnp.dot(z_ref[m:m + mt, :], wd_ref[0], preferred_element_type=F32)
            y_ref[m:m + mt, :] = (h_ref[m:m + mt, :].astype(F32) + acc).astype(BF16)


def mlp(layer, r, wu, wd, h, tn=512, td=256, mt=1024):
    rows, d = r.shape
    ff = wu.shape[2]
    n_up = ff // tn
    n_dn = d // td
    return pl.pallas_call(
        functools.partial(mlp_body, n_up, tn, mt),
        grid=(n_up + n_dn,),
        in_specs=[
            pl.BlockSpec((rows, d), lambda i: (0, 0), pipeline_mode=pl.Buffered(1)),
            pl.BlockSpec((1, d, tn), lambda i: (layer, 0, jnp.minimum(i, n_up - 1))),
            pl.BlockSpec((1, ff, td), lambda i: (layer, 0, jnp.maximum(i - n_up, 0))),
            pl.BlockSpec((rows, td), lambda i: (0, jnp.maximum(i - n_up, 0))),
        ],
        out_specs=pl.BlockSpec((rows, td), lambda i: (0, jnp.maximum(i - n_up, 0))),
        out_shape=jax.ShapeDtypeStruct((rows, d), BF16),
        scratch_shapes=[pltpu.VMEM((rows, ff), BF16)],
        compiler_params=params(),
        cost_estimate=cost(4 * rows * d * ff, 4 * ff * d),
        name="mlp",
    )(r, wu, wd, h)


def solution(mesh):
    tok_spec = P(None, ("data", "seq"), None)
    in_specs = (tok_spec, P(("data", "seq"))) + (P(),) * 8

    def device_fn(x_loc, pos_loc, w_query, w_key, w_value, w_out, w_up, w_down, g_attn, g_mlp):
        n_layers, d, n_heads, head_dim = w_query.shape
        n_kv = w_key.shape[2]
        n_batch, s, _ = x_loc.shape
        rows = n_batch * s
        half = head_dim // 2
        inv_freq = ROPE_BASE ** (-jnp.arange(half, dtype=F32) * (2.0 / head_dim))
        angles = inv_freq[:, None] * pos_loc.astype(F32)[None, :]
        cos, sin = jnp.cos(angles), jnp.sin(angles)
        wq = jnp.transpose(w_query, (0, 2, 3, 1)).reshape(n_layers, n_heads * head_dim, d)
        wk = jnp.transpose(w_key, (0, 2, 3, 1)).reshape(n_layers, n_kv * head_dim, d)
        wv = jnp.transpose(w_value, (0, 2, 3, 1)).reshape(n_layers, n_kv * head_dim, d)
        wo = w_out.reshape(n_layers, n_heads * head_dim, d)
        x = x_loc.reshape(rows, d)
        for layer in range(n_layers):
            n, kv = kv_proj(layer, x, g_attn, wk, wv, cos, sin, head_dim, n_batch)
            o = q_attention(layer, n, wq, cos, sin, kv, head_dim, n_kv)
            h, r = out_proj(layer, o.reshape(rows, n_heads * head_dim), wo, x, g_mlp)
            x = mlp(layer, r, w_up, w_down, h)
        return x.reshape(x_loc.shape)

    return jax.shard_map(device_fn, mesh=mesh, in_specs=in_specs, out_specs=tok_spec, check_vma=False)
```
